256 devices in a mesh: band: 4 (over x, y), tm: 64 (over z, core).
Axes of the slice: x: 2, y: 2, z: 32, core: 2. Of those that a mesh axis runs over, the one named last changes fastest.
The devices are a block of a 4x8x32 slice.
Arguments:
- voltages: bfloat16 [32, 2, 512, 16384], P('band', None, None, 'tm'), parts along dimension 0, may hold values from -12 to 12
- antenna_flags: int32 [128, 32], P('tm', 'band'), parts along dimension 1, may hold values from -2147483648 to 2147483647, as said below
- owned_tile: int32 [64], replicated, may hold values from 0 to 63, each once
Outputs:
- visibility: float32 [512, 32, 2, 512], P('tm', 'band'), parts along dimension 1
The draws below stay inside these ranges and needn't reach their ends.
There are 4 independent parts, one for each index of `band`. The reference program is written for one: setup_inputs(seed, part) draws one part's arguments, and reference() takes and returns one part's arrays. A program takes and returns all parts, laid end to end along the dimension named above; an argument that names none is the same for every part. Nothing has to cross between parts.
Inputs may be any that keep to these rules, and one draw needn't show every extreme that they name: `antenna_flags`: bit b of word w of sub-integration s is 1 where the samples of both polarisations of antenna 32 * w + b are good in that sub-integration of 128 samples, 0 where flagged; all 32 bits of a word are used; some antennas may be flagged in every sub-integration. A permutation: the index k of tm holds the baseline rows of tile owned_tile[k].
All inputs are finite; a program needn't handle non-finite values.
Results may differ from the reference program's by a relative error of at most 0.0003.
Values sent between devices are 32-bit elements; how exact they have to be, the bound alone decides.
No kernel may reach another device: no remote copies, remote signals or barrier semaphores. Data moves between devices by JAX's collectives and lax.ppermute only.
A program may use at most 128 MiB of HBM per device.

```python
import math
import jax
import jax.numpy as jnp
from jax import lax

ANTENNAS = 256
INPUTS = 512
FLAG_WORDS = 8
CHANS = 8
SAMPLES_DEV = 256
SUB_LEN = 128
SUBS = 128
TIME = 16384
TILES = 64
N_TM = 64


def gains(key, lowest, highest):
    key_amplitude, key_phase = jax.random.split(key)
    amplitude = jnp.exp(jax.random.uniform(key_amplitude, (INPUTS,), jnp.float32, math.log(lowest), math.log(highest)))
    phase = jax.random.uniform(key_phase, (INPUTS,), jnp.float32, -math.pi, math.pi)
    return (amplitude * jnp.cos(phase), amplitude * jnp.sin(phase))


def source_term(key, lowest, highest):
    key_sky, key_gain = jax.random.split(key)
    sky = jax.random.normal(key_sky, (CHANS, 2, 1, TIME), jnp.float32)
    gain_real, gain_imag = gains(key_gain, lowest, highest)
    gain_real = gain_real[None, :, None]
    gain_imag = gain_imag[None, :, None]
    real_term = gain_real * sky[:, 0] - gain_imag * sky[:, 1]
    imag_term = gain_real * sky[:, 1] + gain_imag * sky[:, 0]
    return jnp.stack([real_term, imag_term], axis=1)


def draw_voltages(key, part):
    key_first = jax.random.fold_in(jax.random.fold_in(key, 11), 0)
    key_noise = jax.random.fold_in(jax.random.fold_in(key, 11), 2)
    noise = jax.random.normal(key_noise, (CHANS, 2, INPUTS, TIME), jnp.float32)
    signal = source_term(key_first, 0.5, 2.0)
    return jnp.clip(signal + noise, -12.0, 12.0).astype(jnp.bfloat16)


def draw_antenna_flags(key, part):
    key_rolled, key_dead = jax.random.split(jax.random.fold_in(key, 23))
    sub_position = jnp.arange(SUBS, dtype=jnp.int32)[:, None]
    threshold = 30 + 60 * sub_position // max(SUBS - 1, 1)
    rolled = jax.random.randint(key_rolled, (SUBS, ANTENNAS), 0, 100)
    ranking = jax.random.permutation(key_dead, ANTENNAS)
    alive = ranking >= max(1, ANTENNAS // 64)
    bits = jnp.where(alive[None, :] & (rolled < threshold), 1, 0).astype(jnp.int32)
    bits = bits.reshape(SUBS, FLAG_WORDS, 32)
    shifts = jnp.arange(32, dtype=jnp.int32)
    return jnp.sum(jnp.left_shift(bits, shifts[None, None, :]), axis=-1, dtype=jnp.int32)


def setup_inputs(seed: int = 0, part: int = 0) -> dict:
    key_list = jax.random.split(jax.random.key(seed), 4)
    own_keys = jax.random.split(jax.random.fold_in(key_list[3], part), 4)
    voltages = draw_voltages(jax.random.fold_in(jax.random.fold_in(key_list[3], part), 71), part)
    antenna_flags = draw_antenna_flags(jax.random.fold_in(jax.random.fold_in(key_list[3], part), 71), part)
    owned_tile = jax.random.permutation(key_list[2], TILES).astype(jnp.int32)
    return {"voltages": voltages, "antenna_flags": antenna_flags, "owned_tile": owned_tile}


def unpack_flags(words):
    shifts = jnp.arange(32, dtype=jnp.int32)
    bits = jnp.bitwise_and(jnp.right_shift(words[:, :, None], shifts[None, None, :]), 1)
    return bits.reshape(words.shape[0], words.shape[1] * 32).astype(jnp.int32)


def reference(voltages, antenna_flags, owned_tile):
    channels = voltages.shape[0]
    inputs = voltages.shape[2]
    block_rows = inputs // N_TM
    good = unpack_flags(antenna_flags)
    input_flags = jnp.repeat(good, 2, axis=1)
    sample_flags = jnp.repeat(input_flags.T, SUB_LEN, axis=1).astype(jnp.bfloat16)
    masked = voltages * sample_flags[None, None]

    def add_block(running, block_index):
        segment = lax.dynamic_slice_in_dim(masked, block_index * SAMPLES_DEV, SAMPLES_DEV, 3).astype(jnp.float32)
        real_part = segment[:, 0]
        imag_part = segment[:, 1]
        right_side = jnp.concatenate([real_part, imag_part], axis=-1)
        left_side = jnp.stack([right_side, jnp.concatenate([imag_part, -real_part], axis=-1)], axis=1)
        return running + jnp.einsum("ckiu,cju->ckij", left_side, right_side), None

    initial = jnp.zeros((channels, 2, inputs, inputs), jnp.float32)
    gram = lax.scan(add_block, initial, jnp.arange(N_TM, dtype=jnp.int32))[0]
    counts = SUB_LEN * jnp.dot(good.T, good)
    row_index = (owned_tile[:, None] * block_rows + jnp.arange(block_rows, dtype=jnp.int32)[None, :]).reshape(-1)
    pair_counts = jnp.repeat(jnp.repeat(counts, 2, axis=0), 2, axis=1)[row_index]
    ordered = jnp.transpose(gram[:, :, row_index, :], (2, 0, 1, 3))
    return ordered / jnp.maximum(pair_counts, 1).astype(jnp.float32)[:, None, None, :]
```

```python
import functools

import jax
import jax.numpy as jnp
from jax import lax
from jax.experimental import pallas as pl
from jax.experimental.pallas import tpu as pltpu
from jax.sharding import Mesh
from jax.sharding import PartitionSpec as P

LANES = 128
SUBLANES = 8
WORD = 32
CHUNKS = (1, 4)
STREAMS = 4
EARLY = 1


class TableView:
    def __init__(self, ref, begin, shape):
        self.ref, self.begin, self.shape = ref, begin, shape

    def __getitem__(self, at):
        at = at if isinstance(at, tuple) else (at,)
        flat = 0
        for size, i in zip(self.shape, at, strict=True):
            flat = flat * size + i
        return self.ref[self.begin + flat]


def flag_bits(words, sub, bit):
    return jnp.concatenate([(words[sub, w] >> bit) & 1 for w in range(words.shape[1])], axis=0)


def column_bits(words, sub, half):
    lane = lax.broadcasted_iota(jnp.int32, (SUBLANES, LANES), 1)
    first = half * (LANES // WORD)
    word = jnp.full((SUBLANES, LANES), words[sub, first], jnp.int32)
    for w in range(1, LANES // WORD):
        word = jnp.where(lane // WORD == w, words[sub, first + w], word)
    return (word >> (lane % WORD)) & 1


def local_kernel(chips, span, chunks, words_shape, table_ref, volt_ref, mine_ref, own_ref, *rest):
    theirs_refs = rest[: len(chunks)]
    volt, gram, pairs, sems = rest[len(chunks) :]
    channels, _, inputs, samples = volt.shape
    copies = [pltpu.make_async_copy(volt_ref.at[c], volt.at[c], sems.at[c]) for c in range(channels)]
    for copy in copies:
        copy.start()
    z = table_ref[0]
    sign = 1 - 2 * table_ref[1]
    tiles = TableView(table_ref, 2, (2 * chips,))
    words = TableView(table_ref, 2 + 2 * chips, words_shape)
    subs = words_shape[0]
    row = lax.broadcasted_iota(jnp.int32, (inputs // words_shape[1], LANES), 0)
    mask = jnp.concatenate([flag_bits(words, s, (row // 2) % WORD) for s in range(subs)], axis=1)
    mask = mask.astype(jnp.float32).astype(jnp.bfloat16)
    lane_tiles = inputs // LANES

    bit = 4 * (row // SUBLANES) + row % 4
    in_half = (lax.broadcasted_iota(jnp.int32, (inputs, LANES), 0) // 4) % 2
    total = jnp.zeros((inputs, LANES), jnp.int32)
    for s in range(subs):
        lower = jnp.concatenate([column_bits(words, s, 0)] * (inputs // SUBLANES), axis=0)
        upper = jnp.concatenate([column_bits(words, s, 1)] * (inputs // SUBLANES), axis=0)
        total += flag_bits(words, s, bit) * jnp.where(in_half == 0, lower, upper)
    pairs[...] = (total * (samples // subs)).astype(jnp.float32)

    def place(c, slot, ref, at, side):
        chip = (z + side * sign * (span - slot) + chips) % chips
        for h in range(2):
            first = pl.multiple_of(tiles[2 * chip + h] * SUBLANES, SUBLANES)
            if c is None:
                ref[at, h, :SUBLANES, :] = pairs[pl.ds(first, SUBLANES), :]
                continue
            for p in range(2):
                for n in range(lane_tiles):
                    at_row = (((c * 2 + p) * lane_tiles + n) + 1) * SUBLANES
                    ref[at, h, at_row : at_row + SUBLANES, :] = gram[
                        p, pl.ds(first, SUBLANES), n * LANES : (n + 1) * LANES
                    ]

    def place_all(c):
        def own(slot, carry):
            place(c, slot, mine_ref, slot, 1)
            return carry

        lax.fori_loop(0, span, own, 0)
        place(c, span, own_ref, 0, 1)
        begin = 0
        for ref, size in zip(theirs_refs, chunks, strict=True):

            def other(slot, carry, ref=ref, begin=begin):
                place(c, slot + begin, ref, slot, -1)
                return carry

            lax.fori_loop(0, size, other, 0)
            begin += size

    place_all(None)
    for c in range(channels):
        copies[c].wait()
        real = volt[c, 0] * mask
        imag = volt[c, 1] * mask
        right = jnp.concatenate([real, imag], axis=1)
        turned = jnp.concatenate([imag, -real], axis=1)
        for p, left in enumerate((right, turned)):
            gram[p] = lax.dot_general(left, right, (((1,), (1,)), ((), ())), preferred_element_type=jnp.float32)
        place_all(c)


def local_grams(chips, span, chunks, words_shape, table, voltages):
    channels, parts, inputs, samples = voltages.shape
    height = (channels * parts * (inputs // LANES) + 1) * SUBLANES
    vmem = pl.BlockSpec(memory_space=pltpu.VMEM)
    sizes = (span, 1, *chunks)
    return pl.pallas_call(
        functools.partial(local_kernel, chips, span, chunks, words_shape),
        name="grams",
        out_shape=[jax.ShapeDtypeStruct((size, 2, height, LANES), jnp.float32) for size in sizes],
        in_specs=[pl.BlockSpec(memory_space=pltpu.SMEM), pl.BlockSpec(memory_space=pltpu.HBM)],
        out_specs=[vmem] * len(sizes),
        scratch_shapes=[
            pltpu.VMEM((channels, parts, inputs, samples), jnp.bfloat16),
            pltpu.VMEM((parts, inputs, inputs), jnp.float32),
            pltpu.VMEM((inputs, LANES), jnp.float32),
            pltpu.SemaphoreType.DMA((channels,)),
        ],
        compiler_params=pltpu.CompilerParams(vmem_limit_bytes=32 * 2**20),
    )(table, pltpu.with_memory_space_constraint(voltages, pltpu.HBM))


def add_kernel(parts, begin, received_ref, *rest):
    out_ref = rest[-1]
    rows = pl.ds(begin, out_ref.shape[1])
    total = None if received_ref is None else received_ref[...]
    for ref, slot in zip(rest, parts, strict=False):
        piece = ref[slot, :, rows, :]
        total = piece if total is None else total + piece
    out_ref[...] = total


def add(received, parts, begin, rows):
    vmem = pl.BlockSpec(memory_space=pltpu.VMEM)
    operands = [array for array, _ in parts]
    body = functools.partial(add_kernel, [slot for _, slot in parts], begin)
    if received is None:
        body = functools.partial(body, None)
    else:
        operands = [received, *operands]
    return pl.pallas_call(
        body,
        name="add",
        out_shape=jax.ShapeDtypeStruct((2, rows, LANES), jnp.float32),
        in_specs=[vmem] * len(operands),
        out_specs=vmem,
        compiler_params=pltpu.CompilerParams(vmem_limit_bytes=2**20),
    )(*(pltpu.with_memory_space_constraint(o, pltpu.VMEM) for o in operands))


def last_add_kernel(begin, table_ref, received_ref, own_ref, keep_ref, send_ref):
    core = table_ref[1]
    rows = pl.ds(begin, keep_ref.shape[0])
    keep_ref[...] = received_ref[core] + own_ref[0, core, rows, :]
    send_ref[...] = received_ref[1 - core] + own_ref[0, 1 - core, rows, :]


def last_add(table, received, own, begin, rows):
    vmem = pl.BlockSpec(memory_space=pltpu.VMEM)
    return pl.pallas_call(
        functools.partial(last_add_kernel, begin),
        name="last_add",
        out_shape=[jax.ShapeDtypeStruct((rows, LANES), jnp.float32)] * 2,
        in_specs=[pl.BlockSpec(memory_space=pltpu.SMEM), vmem, vmem],
        out_specs=[vmem] * 2,
        compiler_params=pltpu.CompilerParams(vmem_limit_bytes=2**20),
    )(table, *(pltpu.with_memory_space_constraint(o, pltpu.VMEM) for o in (received, own)))


def shards(voltages, antenna_flags, owned_tile):
    chips = lax.axis_size("z")
    core = lax.axis_index("core")
    place = jnp.stack([lax.axis_index("z"), core]).astype(jnp.int32)
    channels = voltages.shape[0]
    inputs = voltages.shape[2]
    lane_tiles = inputs // LANES
    span = (chips + EARLY) // 2
    onward = [(2 * z, 2 * ((z + 1) % chips)) for z in range(chips)]
    back = [(2 * z + 1, 2 * ((z - 1) % chips) + 1) for z in range(chips)]
    swap = [(0, 1), (1, 0)]
    chunks = CHUNKS
    chunks = (*chunks, span - sum(chunks))
    share = channels // STREAMS * 2 * lane_tiles * SUBLANES
    begins = [0, *(SUBLANES + share * s for s in range(1, STREAMS))]
    rows = [share + SUBLANES, *([share] * (STREAMS - 1))]

    table = jnp.concatenate([place, owned_tile, antenna_flags.reshape(-1)])
    mine, own, *others = local_grams(chips, span, chunks, antenna_flags.shape, table, voltages)
    theirs = [lax.ppermute(others[0], "core", swap)]
    message = [add(None, [(mine, 0), (theirs[0], 0)], b, r) for b, r in zip(begins, rows, strict=True)]
    arrived = message[0]
    for other in others[1:]:
        other, _ = lax.optimization_barrier((other, arrived))
        arrived = lax.ppermute(other, "core", swap)
        theirs.append(arrived)

    def parts_of(slot):
        begin = 0
        for part, size in zip(theirs, chunks, strict=True):
            if slot < begin + size:
                return [(mine, slot), (part, slot - begin)]
            begin += size

    for step in range(span):
        pairs = back if step < EARLY else back + onward
        for s in range(STREAMS):
            received = lax.ppermute(message[s], ("z", "core"), pairs)
            if step + 1 < span:
                message[s] = add(received, parts_of(step + 1), begins[s], rows[s])
            else:
                message[s] = last_add(table, received, own, begins[s], rows[s])

    tiles = [keep + lax.ppermute(send, "core", swap) for keep, send in message]
    pairs = tiles[0][:SUBLANES].reshape(2, 4, LANES)
    counts = jnp.moveaxis(pairs, 0, 1).reshape(4, 2 * LANES)
    divisor = jnp.maximum(jnp.repeat(jnp.repeat(counts, 2, axis=0), 2, axis=1), 1.0)
    tiles[0] = tiles[0][SUBLANES:]
    grams = jnp.concatenate([t.reshape(-1, 2, lane_tiles, SUBLANES, LANES) for t in tiles], axis=0)
    ordered = grams.transpose(3, 0, 1, 2, 4).reshape(SUBLANES, channels, 2, inputs)
    return ordered / divisor[:, None, None, :]


def solution(mesh):
    tm = mesh.shape["tm"]
    finer = Mesh(mesh.devices.reshape(mesh.shape["band"], tm // 2, 2), ("band", "z", "core"))
    axes = ("z", "core")
    in_specs = (P("band", None, None, axes), P(axes, "band"), P())
    out_specs = P(axes, "band", None, None)
    return jax.shard_map(shards, mesh=finer, in_specs=in_specs, out_specs=out_specs, check_vma=False)
```

```python
import functools

import jax
import jax.numpy as jnp
from jax import lax
from jax.experimental import pallas as pl
from jax.experimental.pallas import tpu as pltpu
from jax.sharding import Mesh
from jax.sharding import PartitionSpec as P

LANES = 128
SUBLANES = 8
WORD = 32
CHUNKS = (1, 4)
STREAMS = 3


def flag_bits(words, sub, bit):
    return jnp.concatenate([(words[sub, w] >> bit) & 1 for w in range(words.shape[1])], axis=0)


def column_bits(words, sub, half):
    lane = lax.broadcasted_iota(jnp.int32, (SUBLANES, LANES), 1)
    first = half * (LANES // WORD)
    word = jnp.full((SUBLANES, LANES), words[sub, first], jnp.int32)
    for w in range(1, LANES // WORD):
        word = jnp.where(lane // WORD == w, words[sub, first + w], word)
    return (word >> (lane % WORD)) & 1


def local_kernel(chips, span, chunks, tiles_hbm, words_hbm, volt_ref, mine_ref, own_ref, *rest):
    theirs_refs = rest[: len(chunks)]
    volt, gram, pairs, tiles, words, sems = rest[len(chunks) :]
    channels, _, inputs, samples = volt.shape
    for c in range(channels):
        pltpu.make_async_copy(volt_ref.at[c], volt.at[c], sems.at[c]).start()
    small = [
        pltpu.make_async_copy(tiles_hbm, tiles, sems.at[channels]),
        pltpu.make_async_copy(words_hbm, words, sems.at[channels + 1]),
    ]
    for copy in small:
        copy.start()
    for copy in small:
        copy.wait()
    z = lax.axis_index("z")
    sign = 1 - 2 * ((z + lax.axis_index("core")) % 2)
    subs = words.shape[0]
    row = lax.broadcasted_iota(jnp.int32, (inputs // words.shape[1], LANES), 0)
    mask = jnp.concatenate([flag_bits(words, s, (row // 2) % WORD) for s in range(subs)], axis=1)
    mask = mask.astype(jnp.float32).astype(jnp.bfloat16)
    lane_tiles = inputs // LANES

    bit = 4 * (row // SUBLANES) + row % 4
    in_half = (lax.broadcasted_iota(jnp.int32, (inputs, LANES), 0) // 4) % 2
    total = jnp.zeros((inputs, LANES), jnp.int32)
    for s in range(subs):
        lower = jnp.concatenate([column_bits(words, s, 0)] * (inputs // SUBLANES), axis=0)
        upper = jnp.concatenate([column_bits(words, s, 1)] * (inputs // SUBLANES), axis=0)
        total += flag_bits(words, s, bit) * jnp.where(in_half == 0, lower, upper)
    pairs[...] = (total * (samples // subs)).astype(jnp.float32)

    def place(c, slot, ref, at, side):
        chip = (z + side * sign * (span - slot) + chips) % chips
        for h in range(2):
            first = pl.multiple_of(tiles[2 * chip + h] * SUBLANES, SUBLANES)
            if c is None:
                ref[at, h, :SUBLANES, :] = pairs[pl.ds(first, SUBLANES), :]
                continue
            for p in range(2):
                for n in range(lane_tiles):
                    at_row = pl.multiple_of((((c * 2 + p) * lane_tiles + n) + 1) * SUBLANES, SUBLANES)
                    ref[at, h, pl.ds(at_row, SUBLANES), :] = gram[
                        pl.ds(p * inputs + first, SUBLANES), n * LANES : (n + 1) * LANES
                    ]

    def place_all(c):
        for slot in range(span):
            place(c, slot, mine_ref, slot, 1)
        place(c, span, own_ref, 0, 1)
        begin = 0
        for ref, size in zip(theirs_refs, chunks, strict=True):
            for slot in range(size):
                place(c, slot + begin, ref, slot, -1)
            begin += size

    place_all(None)

    def channel(c, carry):
        pltpu.make_async_copy(volt_ref.at[c], volt.at[c], sems.at[c]).wait()
        real = volt[c, 0] * mask
        imag = volt[c, 1] * mask
        right = jnp.concatenate([real, imag], axis=1)
        turned = jnp.concatenate([imag, -real], axis=1)
        left = jnp.concatenate([right, turned], axis=0)
        gram[...] = lax.dot_general(left, right, (((1,), (1,)), ((), ())), preferred_element_type=jnp.float32)
        place_all(c)
        return carry

    lax.fori_loop(0, channels, channel, 0)


def local_grams(chips, span, chunks, owned_tile, words, voltages):
    channels, parts, inputs, samples = voltages.shape
    height = (channels * parts * (inputs // LANES) + 1) * SUBLANES
    vmem = pl.BlockSpec(memory_space=pltpu.VMEM)
    sizes = (span, 1, *chunks)
    return pl.pallas_call(
        functools.partial(local_kernel, chips, span, chunks),
        name="grams",
        out_shape=[jax.ShapeDtypeStruct((size, 2, height, LANES), jnp.float32) for size in sizes],
        in_specs=[pl.BlockSpec(memory_space=pltpu.HBM)] * 3,
        out_specs=[vmem] * len(sizes),
        scratch_shapes=[
            pltpu.VMEM((channels, parts, inputs, samples), jnp.bfloat16),
            pltpu.VMEM((parts * inputs, inputs), jnp.float32),
            pltpu.VMEM((inputs, LANES), jnp.float32),
            pltpu.SMEM(owned_tile.shape, jnp.int32),
            pltpu.SMEM(words.shape, jnp.int32),
            pltpu.SemaphoreType.DMA((channels + 2,)),
        ],
        compiler_params=pltpu.CompilerParams(vmem_limit_bytes=32 * 2**20),
    )(*(pltpu.with_memory_space_constraint(o, pltpu.HBM) for o in (owned_tile, words, voltages)))


def add_kernel(parts, begin, received_ref, *rest):
    out_ref = rest[-1]
    rows = pl.ds(begin, out_ref.shape[1])
    total = None if received_ref is None else received_ref[...]
    for ref, slot in zip(rest, parts, strict=False):
        piece = ref[slot, :, rows, :]
        total = piece if total is None else total + piece
    out_ref[...] = total


def add(received, parts, begin, rows):
    vmem = pl.BlockSpec(memory_space=pltpu.VMEM)
    operands = [array for array, _ in parts]
    body = functools.partial(add_kernel, [slot for _, slot in parts], begin)
    if received is None:
        body = functools.partial(body, None)
    else:
        operands = [received, *operands]
    return pl.pallas_call(
        body,
        name="add",
        out_shape=jax.ShapeDtypeStruct((2, rows, LANES), jnp.float32),
        in_specs=[vmem] * len(operands),
        out_specs=vmem,
        compiler_params=pltpu.CompilerParams(vmem_limit_bytes=2**20),
    )(*(pltpu.with_memory_space_constraint(o, pltpu.VMEM) for o in operands))


def last_add_kernel(*refs):
    *received_refs, own_ref, keep_ref, send_ref = refs
    core = lax.axis_index("core")
    begin = 0
    for ref in received_refs:
        rows = pl.ds(begin, ref.shape[1])
        keep_ref[rows, :] = ref[core] + own_ref[0, core, rows, :]
        send_ref[rows, :] = ref[1 - core] + own_ref[0, 1 - core, rows, :]
        begin += ref.shape[1]


def last_add(received, own):
    operands = [*received, own]
    vmem = pl.BlockSpec(memory_space=pltpu.VMEM)
    return pl.pallas_call(
        last_add_kernel,
        name="last_add",
        out_shape=[jax.ShapeDtypeStruct(own.shape[2:], jnp.float32)] * 2,
        in_specs=[vmem] * len(operands),
        out_specs=[vmem] * 2,
        compiler_params=pltpu.CompilerParams(vmem_limit_bytes=2**20),
    )(*(pltpu.with_memory_space_constraint(o, pltpu.VMEM) for o in operands))


def shards(voltages, antenna_flags, owned_tile):
    chips = lax.axis_size("z")
    channels = voltages.shape[0]
    inputs = voltages.shape[2]
    lane_tiles = inputs // LANES
    span = chips // 2
    ahead = [(z + 1) % chips for z in range(chips)]
    behind = [(z - 1) % chips for z in range(chips)]
    onward = [(2 * z + z % 2, 2 * t + t % 2) for z, t in enumerate(ahead)]
    back = [(2 * z + 1 - z % 2, 2 * t + 1 - t % 2) for z, t in enumerate(behind)]
    swap = [(0, 1), (1, 0)]
    chunks = CHUNKS
    chunks = (*chunks, span - sum(chunks))
    height = channels * 2 * lane_tiles + 1
    begins = [height * s // STREAMS * SUBLANES for s in range(STREAMS + 1)]
    rows = [end - begin for begin, end in zip(begins, begins[1:])]

    mine, own, *others = local_grams(chips, span, chunks, owned_tile, antenna_flags, voltages)
    theirs = []
    for other in others:
        theirs.append(lax.ppermute(other, "core", swap))
    message = [add(None, [(mine, 0), (theirs[0], 0)], b, r) for b, r in zip(begins, rows)]

    def parts_of(slot):
        begin = 0
        for part, size in zip(theirs, chunks, strict=True):
            if slot < begin + size:
                return [(mine, slot), (part, slot - begin)]
            begin += size

    for step in range(span):
        for s in range(STREAMS):
            pairs = onward + back if step > 0 else back if s % 2 else onward
            received = lax.ppermute(message[s], ("z", "core"), pairs)
            if step + 1 < span:
                message[s] = add(received, parts_of(step + 1), begins[s], rows[s])
            else:
                message[s] = received

    keep, send = last_add(message, own)
    tile = keep + lax.ppermute(send, "core", swap)
    pairs = tile[:SUBLANES].reshape(2, 4, LANES)
    counts = jnp.moveaxis(pairs, 0, 1).reshape(4, 2 * LANES)
    divisor = jnp.maximum(jnp.repeat(jnp.repeat(counts, 2, axis=0), 2, axis=1), 1.0)
    grams = tile[SUBLANES:].reshape(channels, 2, lane_tiles, SUBLANES, LANES)
    ordered = grams.transpose(3, 0, 1, 2, 4).reshape(SUBLANES, channels, 2, inputs)
    return ordered / divisor[:, None, None, :]


def solution(mesh):
    tm = mesh.shape["tm"]
    finer = Mesh(mesh.devices.reshape(mesh.shape["band"], tm // 2, 2), ("band", "z", "core"))
    axes = ("z", "core")
    in_specs = (P("band", None, None, axes), P(axes, "band"), P())
    out_specs = P(axes, "band", None, None)
    return jax.shard_map(shards, mesh=finer, in_specs=in_specs, out_specs=out_specs, check_vma=False)
```

```python
import functools

import jax
import jax.numpy as jnp
from jax import lax
from jax.experimental import pallas as pl
from jax.experimental.pallas import tpu as pltpu
from jax.sharding import Mesh
from jax.sharding import PartitionSpec as P

LANES = 128
SUBLANES = 8
WORD = 32
CHUNKS = (1, 4)
STREAMS = 3


def flag_bits(words, sub, bit):
    return jnp.concatenate([(words[sub, w] >> bit) & 1 for w in range(words.shape[1])], axis=0)


def column_bits(words, sub, half):
    lane = lax.broadcasted_iota(jnp.int32, (SUBLANES, LANES), 1)
    first = half * (LANES // WORD)
    word = jnp.full((SUBLANES, LANES), words[sub, first], jnp.int32)
    for w in range(1, LANES // WORD):
        word = jnp.where(lane // WORD == w, words[sub, first + w], word)
    return (word >> (lane % WORD)) & 1


def local_kernel(chips, span, chunks, tiles_hbm, words_hbm, volt_ref, mine_ref, own_ref, *rest):
    theirs_refs = rest[: len(chunks)]
    volt, gram, pairs, tiles, words, sems = rest[len(chunks) :]
    channels, _, inputs, samples = volt.shape
    for c in range(channels):
        pltpu.make_async_copy(volt_ref.at[c], volt.at[c], sems.at[c]).start()
    small = [
        pltpu.make_async_copy(tiles_hbm, tiles, sems.at[channels]),
        pltpu.make_async_copy(words_hbm, words, sems.at[channels + 1]),
    ]
    for copy in small:
        copy.start()
    for copy in small:
        copy.wait()
    z = lax.axis_index("z")
    sign = 1 - 2 * ((z + lax.axis_index("core")) % 2)
    subs = words.shape[0]
    row = lax.broadcasted_iota(jnp.int32, (inputs // words.shape[1], LANES), 0)
    mask = jnp.concatenate([flag_bits(words, s, (row // 2) % WORD) for s in range(subs)], axis=1)
    mask = mask.astype(jnp.float32).astype(jnp.bfloat16)
    lane_tiles = inputs // LANES

    bit = 4 * (row // SUBLANES) + row % 4
    in_half = (lax.broadcasted_iota(jnp.int32, (inputs, LANES), 0) // 4) % 2
    total = jnp.zeros((inputs, LANES), jnp.int32)
    for s in range(subs):
        lower = jnp.concatenate([column_bits(words, s, 0)] * (inputs // SUBLANES), axis=0)
        upper = jnp.concatenate([column_bits(words, s, 1)] * (inputs // SUBLANES), axis=0)
        total += flag_bits(words, s, bit) * jnp.where(in_half == 0, lower, upper)
    pairs[...] = (total * (samples // subs)).astype(jnp.float32)

    def place(c, slot, ref, at, side):
        chip = (z + side * sign * (span - slot) + chips) % chips
        for h in range(2):
            first = pl.multiple_of(tiles[2 * chip + h] * SUBLANES, SUBLANES)
            if c is None:
                ref[at, h, :SUBLANES, :] = pairs[pl.ds(first, SUBLANES), :]
                continue
            for p in range(2):
                for n in range(lane_tiles):
                    at_row = pl.multiple_of((((c * 2 + p) * lane_tiles + n) + 1) * SUBLANES, SUBLANES)
                    ref[at, h, pl.ds(at_row, SUBLANES), :] = gram[
                        pl.ds(p * inputs + first, SUBLANES), n * LANES : (n + 1) * LANES
                    ]

    def place_all(c):
        for slot in range(span):
            place(c, slot, mine_ref, slot, 1)
        place(c, span, own_ref, 0, 1)
        begin = 0
        for ref, size in zip(theirs_refs, chunks, strict=True):
            for slot in range(size):
                place(c, slot + begin, ref, slot, -1)
            begin += size

    place_all(None)

    def channel(c, carry):
        pltpu.make_async_copy(volt_ref.at[c], volt.at[c], sems.at[c]).wait()
        real = volt[c, 0] * mask
        imag = volt[c, 1] * mask
        right = jnp.concatenate([real, imag], axis=1)
        turned = jnp.concatenate([imag, -real], axis=1)
        left = jnp.concatenate([right, turned], axis=0)
        gram[...] = lax.dot_general(left, right, (((1,), (1,)), ((), ())), preferred_element_type=jnp.float32)
        place_all(c)
        return carry

    lax.fori_loop(0, channels, channel, 0)


def local_grams(chips, span, chunks, owned_tile, words, voltages):
    channels, parts, inputs, samples = voltages.shape
    height = (channels * parts * (inputs // LANES) + 1) * SUBLANES
    vmem = pl.BlockSpec(memory_space=pltpu.VMEM)
    sizes = (span, 1, *chunks)
    return pl.pallas_call(
        functools.partial(local_kernel, chips, span, chunks),
        name="grams",
        out_shape=[jax.ShapeDtypeStruct((size, 2, height, LANES), jnp.float32) for size in sizes],
        in_specs=[pl.BlockSpec(memory_space=pltpu.HBM)] * 3,
        out_specs=[vmem] * len(sizes),
        scratch_shapes=[
            pltpu.VMEM((channels, parts, inputs, samples), jnp.bfloat16),
            pltpu.VMEM((parts * inputs, inputs), jnp.float32),
            pltpu.VMEM((inputs, LANES), jnp.float32),
            pltpu.SMEM(owned_tile.shape, jnp.int32),
            pltpu.SMEM(words.shape, jnp.int32),
            pltpu.SemaphoreType.DMA((channels + 2,)),
        ],
        compiler_params=pltpu.CompilerParams(vmem_limit_bytes=32 * 2**20),
    )(*(pltpu.with_memory_space_constraint(o, pltpu.HBM) for o in (owned_tile, words, voltages)))


def add_kernel(parts, begin, one_way, received_ref, *rest):
    out_ref = rest[-1]
    rows = pl.ds(begin, out_ref.shape[1])
    total = None if received_ref is None else received_ref[...]
    if one_way is not None:
        way = (lax.axis_index("z") + lax.axis_index("core")) % 2
        total = jnp.where(way == one_way, total, 0.0)
    for ref, slot in zip(rest, parts, strict=False):
        piece = ref[slot, :, rows, :]
        total = piece if total is None else total + piece
    out_ref[...] = total


def add(received, parts, begin, rows, one_way=None):
    vmem = pl.BlockSpec(memory_space=pltpu.VMEM)
    operands = [array for array, _ in parts]
    body = functools.partial(add_kernel, [slot for _, slot in parts], begin, one_way)
    if received is None:
        body = functools.partial(body, None)
    else:
        operands = [received, *operands]
    return pl.pallas_call(
        body,
        name="add",
        out_shape=jax.ShapeDtypeStruct((2, rows, LANES), jnp.float32),
        in_specs=[vmem] * len(operands),
        out_specs=vmem,
        compiler_params=pltpu.CompilerParams(vmem_limit_bytes=2**20),
    )(*(pltpu.with_memory_space_constraint(o, pltpu.VMEM) for o in operands))


def last_add_kernel(*refs):
    *received_refs, own_ref, keep_ref, send_ref = refs
    core = lax.axis_index("core")
    begin = 0
    for ref in received_refs:
        rows = pl.ds(begin, ref.shape[1])
        keep_ref[rows, :] = ref[core] + own_ref[0, core, rows, :]
        send_ref[rows, :] = ref[1 - core] + own_ref[0, 1 - core, rows, :]
        begin += ref.shape[1]


def last_add(received, own):
    operands = [*received, own]
    vmem = pl.BlockSpec(memory_space=pltpu.VMEM)
    return pl.pallas_call(
        last_add_kernel,
        name="last_add",
        out_shape=[jax.ShapeDtypeStruct(own.shape[2:], jnp.float32)] * 2,
        in_specs=[vmem] * len(operands),
        out_specs=[vmem] * 2,
        compiler_params=pltpu.CompilerParams(vmem_limit_bytes=2**20),
    )(*(pltpu.with_memory_space_constraint(o, pltpu.VMEM) for o in operands))


def shards(voltages, antenna_flags, owned_tile):
    chips = lax.axis_size("z")
    channels = voltages.shape[0]
    inputs = voltages.shape[2]
    lane_tiles = inputs // LANES
    span = chips // 2
    ahead = [(z + 1) % chips for z in range(chips)]
    behind = [(z - 1) % chips for z in range(chips)]
    onward = [(2 * z + z % 2, 2 * t + t % 2) for z, t in enumerate(ahead)]
    back = [(2 * z + 1 - z % 2, 2 * t + 1 - t % 2) for z, t in enumerate(behind)]
    swap = [(0, 1), (1, 0)]
    chunks = CHUNKS
    chunks = (*chunks, span - sum(chunks))
    height = channels * 2 * lane_tiles + 1
    begins = [height * s // STREAMS * SUBLANES for s in range(STREAMS + 1)]
    rows = [end - begin for begin, end in zip(begins, begins[1:])]

    mine, own, *others = local_grams(chips, span, chunks, owned_tile, antenna_flags, voltages)
    theirs = []
    for other in others:
        theirs.append(lax.ppermute(other, "core", swap))
    message = [add(None, [(mine, 0), (theirs[0], 0)], b, r) for b, r in zip(begins, rows)]

    def parts_of(slot):
        begin = 0
        for part, size in zip(theirs, chunks, strict=True):
            if slot < begin + size:
                return [(mine, slot), (part, slot - begin)]
            begin += size

    for step in range(span):
        for s in range(STREAMS):
            pairs = onward + back if step > 0 or s == 0 else back if s % 2 else onward
            received = lax.ppermute(message[s], ("z", "core"), pairs)
            if step + 1 < span:
                one_way = 0 if step == 0 and s == 0 else None
                message[s] = add(received, parts_of(step + 1), begins[s], rows[s], one_way)
            else:
                message[s] = received

    keep, send = last_add(message, own)
    tile = keep + lax.ppermute(send, "core", swap)
    pairs = tile[:SUBLANES].reshape(2, 4, LANES)
    counts = jnp.moveaxis(pairs, 0, 1).reshape(4, 2 * LANES)
    divisor = jnp.maximum(jnp.repeat(jnp.repeat(counts, 2, axis=0), 2, axis=1), 1.0)
    grams = tile[SUBLANES:].reshape(channels, 2, lane_tiles, SUBLANES, LANES)
    ordered = grams.transpose(3, 0, 1, 2, 4).reshape(SUBLANES, channels, 2, inputs)
    return ordered / divisor[:, None, None, :]


def solution(mesh):
    tm = mesh.shape["tm"]
    finer = Mesh(mesh.devices.reshape(mesh.shape["band"], tm // 2, 2), ("band", "z", "core"))
    axes = ("z", "core")
    in_specs = (P("band", None, None, axes), P(axes, "band"), P())
    out_specs = P(axes, "band", None, None)
    return jax.shard_map(shards, mesh=finer, in_specs=in_specs, out_specs=out_specs, check_vma=False)
```
